512 devices in a mesh: dp: 8 (over z), vocab: 64 (over x, y, core).
Axes of the slice: x: 4, y: 8, z: 8, core: 2. Of those that a mesh axis runs over, the one named last changes fastest.
Arguments:
- pooled_grad: bfloat16 [16384, 1024], P(('dp', 'vocab')), may hold values from -12 to 12
- token_ids: int32 [16384, 16], P(('dp', 'vocab')), may hold values from 0 to 131071, as said below
Outputs:
- table_grad: float32 [131072, 1024], P(('dp', 'vocab'))
The draws below stay inside these ranges and needn't reach their ends.
Inputs may be any that keep to these rules, and one draw needn't show every extreme that they name: `token_ids`: the owner of id r is (r // 256) % 64. Among the ids of one device's 32 positions at most 24 have the same owner; in every group of 64 devices along vocab some owner gets exactly 24 ids from each of them.
All inputs are finite; a program needn't handle non-finite values.
Results may differ from the reference program's by a relative error of at most 0.0075.
Values may be sent and summed in bfloat16 or wider, within the bound.
A program may use at most 64 MiB of HBM per device.

```python
import jax
import jax.numpy as jnp
from jax import lax

D = 1024
ROWS_DEV = 256
POS_DEV = 32
LIST = 16
GROUPS = 8
OWNERS = 64
CAPACITY = 24
POSITIONS = 16384
VOCAB = 131072
COLUMN_ROWS = 2048


def draw_token_ids(key, part):
    entries = POS_DEV * LIST
    slots_all = OWNERS * CAPACITY
    cand_owner = jnp.arange(slots_all, dtype=jnp.int32) // CAPACITY

    def group_levels(group_key):
        level_key, hot_key = jax.random.split(group_key)
        levels = jax.random.randint(level_key, (OWNERS,), 0, 4, dtype=jnp.int32)
        hottest = jax.random.randint(hot_key, (), 0, OWNERS, dtype=jnp.int32)
        return jnp.where(jnp.arange(OWNERS, dtype=jnp.int32) == hottest, 8, levels)
    group_keys = jax.random.split(jax.random.fold_in(key, 17), GROUPS)
    all_levels = jax.vmap(group_levels)(group_keys)
    device_keys = jax.random.split(jax.random.fold_in(key, 29), GROUPS * OWNERS)

    def device_ids(device_key, levels):
        pick_key, order_key, outer_key, inner_key = jax.random.split(device_key, 4)
        noise = jax.random.randint(pick_key, (slots_all,), 0, 4096, dtype=jnp.int32)
        scores = (levels[cand_owner] * 4096 + noise) * slots_all + jnp.arange(slots_all, dtype=jnp.int32)
        _, chosen = lax.top_k(scores, entries)
        owner_list = cand_owner[chosen]
        owner_list = owner_list[jax.random.permutation(order_key, entries)]
        outer = jax.random.randint(outer_key, (entries,), 0, COLUMN_ROWS, dtype=jnp.int32)
        inner = jax.random.randint(inner_key, (entries,), 0, outer + 1, dtype=jnp.int32)
        return (inner // ROWS_DEV * OWNERS + owner_list) * ROWS_DEV + inner % ROWS_DEV
    device_levels = jnp.repeat(all_levels, OWNERS, axis=0)
    flat_ids = jax.vmap(device_ids)(device_keys, device_levels)
    return flat_ids.reshape(POSITIONS, LIST)


def steps_of(rng, extent, pieces, least, top_value):
    def one(dim, shards_of):
        draws = jax.random.uniform(jax.random.fold_in(jax.random.fold_in(rng, 6), dim), (shards_of,), jnp.float32, least / len(pieces), top_value / len(pieces))
        return jnp.repeat(jnp.exp(draws), extent[dim] // shards_of).reshape((-1,) + (1,) * (len(extent) - dim - 1))

    factor_of = one(*pieces[0])
    for cut in pieces[1:]:
        factor_of = factor_of * one(*cut)
    return factor_of


def gaussian(rng, extent, spread, bound, cuts=(), kind=jnp.bfloat16):
    result = spread * jax.random.normal(rng, extent, jnp.float32)
    if cuts:
        result = result * steps_of(rng, extent, cuts, -0.22, 0.18)
    return jnp.clip(result, -bound, bound).astype(kind)


def setup_inputs(seed: int = 0) -> dict:
    splits = jax.random.split(jax.random.key(seed), 3)
    pooled_grad = gaussian(splits[0], (POSITIONS, D), 2.0, 12.0, ((0, 512),))
    token_ids = draw_token_ids(jax.random.fold_in(splits[2], 71), 0)
    return dict(pooled_grad=pooled_grad, token_ids=token_ids)


def reference(pooled_grad, token_ids):
    id_share = (pooled_grad.astype(jnp.float32) / LIST).astype(jnp.bfloat16)
    width = pooled_grad.shape[1]
    grouped_share = id_share.reshape(GROUPS, -1, width)
    grouped_ids = token_ids.reshape(GROUPS, -1, LIST)

    def add_group(running, inputs):
        shares, id_lists = inputs
        copies = jnp.repeat(shares.astype(jnp.float32), LIST, axis=0)
        partial_value = jax.ops.segment_sum(copies, id_lists.reshape(-1).astype(jnp.int32), num_segments=VOCAB)
        rounded = lax.optimization_barrier(partial_value.astype(jnp.bfloat16))
        return running + rounded.astype(jnp.float32), None

    table_grad, _ = lax.scan(add_group, jnp.zeros((VOCAB, width), jnp.float32), (grouped_share, grouped_ids))
    return table_grad
```

```python
import functools

import jax
import jax.numpy as jnp
from jax import lax
from jax.experimental import pallas as pl
from jax.experimental.pallas import tpu as pltpu
from jax.sharding import PartitionSpec as P

ROWS = 256
LIST = 16
CH = 256
HALF = CH // 2
MESH = pl.DeviceIdType.MESH
MSG = ((4, 0), (3, 1), (3, 0), (2, 1), (2, 0), (1, 1), (1, 0))


def kernel(
    nx, ny, nc, x_hbm, ids_hbm, out_ref,
    x_in, ids_in, xg, ids_x, ids_g, cnt, part, send, got,
    in_sem, id1_s, id1_r, id2_s, id2_r, id3_s, id3_r,
    a1_s, a1_r, b1_s, b1_r, a2_s, a2_r, b2_s, b2_r, p_s, p_r, z_s, z_r,
):
    d = lax.axis_index("dp")
    v = lax.axis_index("vocab")
    c = v % 2
    y = (v // 2) % ny
    x = v // (2 * ny)

    def at(xx, yy, cc):
        return (d, (xx * ny + yy) * 2 + cc)

    xs = [lax.rem(x + k, nx) for k in range(nx)]
    ys = [lax.rem(y + k, ny) for k in range(ny)]
    other = 1 - c
    down = (lax.rem(d + 7, 8), v)
    up = (lax.rem(d + 1, 8), v)

    cp_ids = pltpu.make_async_copy(ids_hbm, ids_in, in_sem.at[0])
    cp_x = pltpu.make_async_copy(x_hbm, x_in, in_sem.at[1])
    cp_ids.start()
    cp_x.start()

    peers = [at(xs[k], y, c) for k in range(1, nx)] + [at(x, ys[k], c) for k in range(1, ny)]
    peers += [at(x, y, other), down, up]
    barrier = pltpu.get_barrier_semaphore()
    for peer in peers:
        pl.semaphore_signal(barrier, inc=1, device_id=peer, device_id_type=MESH)
    cp_ids.wait()
    cp_x.wait()
    for f in range(nc):
        for h in range(2):
            xg[f, c, y, x, h] = x_in[pl.ds(16 * h, 16), pl.ds(CH * f, CH)]
    ids_x[x] = ids_in[...]
    pl.semaphore_wait(barrier, len(peers))

    def rc(src, dst, ss, rs, dev):
        return pltpu.make_async_remote_copy(
            src_ref=src, dst_ref=dst, send_sem=ss, recv_sem=rs, device_id=dev, device_id_type=MESH
        )

    def first(f):
        lanes = pl.ds(CH * f, CH)
        r = []
        for k in range(1, ny):
            r.append(
                rc(x_in.at[pl.ds(16, 16), lanes], xg.at[f, c, y, x, 1], b1_s.at[f, k], b1_r.at[f, k], at(x, ys[k], c))
            )
        for k in range(1, nx):
            r.append(
                rc(x_in.at[pl.ds(0, 16), lanes], xg.at[f, c, y, x, 0], a1_s.at[f, k], a1_r.at[f, k], at(xs[k], y, c))
            )
        return r

    def second(f):
        a = [
            rc(xg.at[f, c, y, :, 0], xg.at[f, c, y, :, 0], a2_s.at[f, k], a2_r.at[f, k], at(x, ys[k], c))
            for k in range(1, ny)
        ]
        b = [
            rc(xg.at[f, c, :, x, 1], xg.at[f, c, :, x, 1], b2_s.at[f, k], b2_r.at[f, k], at(xs[k], y, c))
            for k in range(1, nx)
        ]
        return a, b

    def third(f):
        return rc(xg.at[f, c], xg.at[f, c], p_s.at[f], p_r.at[f], at(x, y, other))

    def start(copies):
        for cp in copies:
            cp.start()

    def arrived(copies):
        for cp in copies:
            cp.wait_recv()

    def sent(copies):
        for cp in copies:
            cp.wait_send()

    def go_second(f):
        arrived(first(f))
        a, b = second(f)
        start(a)
        start(b)

    def go_third(f):
        a, b = second(f)
        arrived(a)
        arrived(b)
        third(f).start()

    id1 = [rc(ids_in, ids_x.at[x], id1_s.at[k], id1_r.at[k], at(xs[k], y, c)) for k in range(1, nx)]
    id2 = [rc(ids_g.at[c, y], ids_g.at[c, y], id2_s.at[k], id2_r.at[k], at(x, ys[k], c)) for k in range(1, ny)]
    id3 = rc(ids_g.at[c], ids_g.at[c], id3_s, id3_r, at(x, y, other))

    start(id1)
    start(first(0))
    arrived(id1)
    lane = lax.broadcasted_iota(jnp.int32, (LIST, 128), 1) // 32
    both = ids_x[0]
    for k in range(1, nx):
        both = jnp.where(lane == k, ids_x[k], both)
    ids_g[c, y] = both
    start(id2)
    go_second(0)
    if nc > 1:
        start(first(1))
    arrived(id2)
    id3.start()
    id3.wait_recv()

    blocks = [lax.rem(d + k, 8) for k in (4, 5, 3, 6, 2, 7, 1, 0)]
    kt = 2 * ny
    row = lax.broadcasted_iota(jnp.int32, (ROWS, 128), 0).astype(jnp.float32).astype(jnp.bfloat16)
    one = jnp.full((ROWS, 128), 1.0 / LIST, jnp.bfloat16)
    zero = jnp.zeros((ROWS, 128), jnp.bfloat16)

    def build(i):
        block = blocks[i]

        def tile(t, _):
            ids = ids_g[t // ny, t % ny]
            hit = (ids // ROWS) == block * (2 * nx * ny) + v
            low = jnp.where(hit, ids % ROWS, -1).astype(jnp.float32).astype(jnp.bfloat16)
            acc = zero
            for j in range(LIST):
                acc = acc + jnp.where(jnp.broadcast_to(low[j : j + 1], (ROWS, 128)) == row, one, zero)
            cnt[i, :, pl.ds(pl.multiple_of(t * 128, 128), 128)] = acc
            return 0

        lax.fori_loop(0, kt, tile, 0)

    def dot(i, f):
        part[i] = jnp.dot(
            cnt[i], xg[f].reshape(kt * 128, CH), preferred_element_type=jnp.float32
        )

    build(0)
    go_third(0)
    build(1)
    build(2)
    third(0).wait_recv()

    def zcopy(way, f, m):
        return rc(
            send.at[way, f, m], got.at[way, f, m], z_s.at[way, f, m], z_r.at[way, f, m], (down, up)[way]
        )

    def part_of(way, m):
        dist, half = MSG[m]
        if way == 1:
            half = 1 - half
        i = 0 if dist == 4 else 2 * (4 - dist) - 1 + way
        return part[i, :, HALF * half : HALF * (half + 1)]

    def finish(f):
        lanes0 = CH * f
        for way in range(2):
            for m in (5, 6):
                zcopy(way, f, m).wait_recv()
        lo = part[7, :, :HALF] + got[0, f, 6].astype(jnp.float32) + got[1, f, 5].astype(jnp.float32)
        hi = part[7, :, HALF:] + got[0, f, 5].astype(jnp.float32) + got[1, f, 6].astype(jnp.float32)
        out_ref[:, pl.ds(pl.multiple_of(lanes0, 128), HALF)] = lo
        out_ref[:, pl.ds(pl.multiple_of(lanes0 + HALF, 128), HALF)] = hi

    def chunk(f, _):
        @pl.when(f > 0)
        def _():
            third(f).wait_recv()

        for i in range(3):
            dot(i, f)
        for m in range(2):
            for way in range(2):
                send[way, f, m] = part_of(way, m).astype(jnp.bfloat16)
                zcopy(way, f, m).start()

        @pl.when(f > 0)
        def _():
            finish(f - 1)

        @pl.when(f + 1 < nc)
        def _():
            go_second(f + 1)

        @pl.when(f + 2 < nc)
        def _():
            start(first(f + 2))

        for i in range(3, 8):
            @pl.when(f == 0)
            def _(i=i):
                build(i)

            dot(i, f)
            if i in (4, 6):
                for m in ((2, 3) if i == 4 else (4,)):
                    for way in range(2):
                        zcopy(way, f, m - 2).wait_recv()
                        send[way, f, m] = (
                            part_of(way, m) + got[way, f, m - 2].astype(jnp.float32)
                        ).astype(jnp.bfloat16)
                        zcopy(way, f, m).start()

        @pl.when(f + 1 < nc)
        def _():
            go_third(f + 1)

        for m in (5, 6):
            for way in range(2):
                zcopy(way, f, m - 2).wait_recv()
                send[way, f, m] = (part_of(way, m) + got[way, f, m - 2].astype(jnp.float32)).astype(
                    jnp.bfloat16
                )
                zcopy(way, f, m).start()
        return 0

    lax.fori_loop(0, nc, chunk, 0)
    finish(nc - 1)

    sent(id1)
    sent(id2)
    id3.wait_send()

    def drain(f, _):
        sent(first(f))
        a, b = second(f)
        sent(a)
        sent(b)
        third(f).wait_send()
        for way in range(2):
            for m in range(7):
                zcopy(way, f, m).wait_send()
        return 0

    lax.fori_loop(0, nc, drain, 0)


def local(nx, ny, pooled_grad, token_ids):
    width = pooled_grad.shape[1]
    nc = width // CH
    ids = jnp.tile(token_ids.T, (1, 4))
    dma = pltpu.SemaphoreType.DMA
    bf = jnp.bfloat16
    return pl.pallas_call(
        functools.partial(kernel, nx, ny, nc),
        out_shape=jax.ShapeDtypeStruct((ROWS, width), jnp.float32),
        in_specs=[pl.BlockSpec(memory_space=pl.ANY)] * 2,
        out_specs=pl.BlockSpec(memory_space=pltpu.VMEM),
        scratch_shapes=[
            pltpu.VMEM((32, width), bf),
            pltpu.VMEM((LIST, 128), jnp.int32),
            pltpu.VMEM((nc, 2, ny, nx, 2, 16, CH), bf),
            pltpu.VMEM((nx, LIST, 128), jnp.int32),
            pltpu.VMEM((2, ny, LIST, 128), jnp.int32),
            pltpu.VMEM((8, ROWS, 2 * ny * 128), bf),
            pltpu.VMEM((8, ROWS, CH), jnp.float32),
            pltpu.VMEM((2, nc, 7, ROWS, HALF), bf),
            pltpu.VMEM((2, nc, 7, ROWS, HALF), bf),
            dma((2,)),
            dma((nx,)), dma((nx,)), dma((ny,)), dma((ny,)), dma, dma,
            dma((nc, nx)), dma((nc, nx)), dma((nc, ny)), dma((nc, ny)),
            dma((nc, ny)), dma((nc, ny)), dma((nc, nx)), dma((nc, nx)),
            dma((nc,)), dma((nc,)), dma((2, nc, 7)), dma((2, nc, 7)),
        ],
        compiler_params=pltpu.CompilerParams(
            collective_id=0, has_side_effects=True, vmem_limit_bytes=60 * 1024 * 1024
        ),
    )(pooled_grad, ids)


def solution(mesh, nx=4, ny=8):
    in_specs = (P(("dp", "vocab"), None), P(("dp", "vocab"), None))
    out_specs = P(("dp", "vocab"), None)
    return jax.shard_map(
        functools.partial(local, nx, ny), mesh=mesh, in_specs=in_specs, out_specs=out_specs, check_vma=False
    )
```

```python
import functools

import jax
import jax.numpy as jnp
from jax import lax
from jax.experimental import pallas as pl
from jax.experimental.pallas import tpu as pltpu
from jax.sharding import PartitionSpec as P

ROWS = 256
HALF = ROWS // 2
LIST = 16
POS = 32
WIDTHS = (128, 256, 256, 256, 128)
OFFS = tuple(sum(WIDTHS[:i]) for i in range(len(WIDTHS)))
NC = len(WIDTHS)
MESH = pl.DeviceIdType.MESH
MSG = ((4, 0), (3, 1), (3, 0), (2, 1), (2, 0), (1, 1), (1, 0))
ROUNDS = ((0, 1), (2, 3), (4, 5), (6,))
BLOCKS = (4, 5, 3, 6, 2, 7, 1, 0)
GROUPS = ((0, 3), (3, 5), (5, 8), (3, 8), (0, 8))


def kernel(nx, ny, x_hbm, ids_hbm, out_hbm, x_in, ids_in, ids_x, ids_g, cnt, *rest):
    xg, part, send, got, outs = (rest[NC * i : NC * (i + 1)] for i in range(5))
    in_sem, out_sem, id_s, id_r, g_s, g_r, z_s, z_r = rest[5 * NC :]
    scope = jax.named_scope
    d = lax.axis_index("dp")
    v = lax.axis_index("vocab")
    c = v % 2
    y = (v // 2) % ny
    x = v // (2 * ny)

    def at(xx, yy, cc):
        return (d, (xx * ny + yy) * 2 + cc)

    xs = [lax.rem(x + k, nx) for k in range(nx)]
    ys = [lax.rem(y + k, ny) for k in range(ny)]
    partner = at(x, y, 1 - c)
    down = (lax.rem(d + 7, 8), v)
    up = (lax.rem(d + 1, 8), v)

    cp_ids = pltpu.make_async_copy(ids_hbm, ids_in, in_sem.at[0])
    cp_x = pltpu.make_async_copy(x_hbm, x_in, in_sem.at[1])
    cp_ids.start()
    cp_x.start()

    peers = [at(x, ys[k], c) for k in range(1, ny)] + [at(xs[k], y, c) for k in range(1, nx)]
    peers += [partner, down, up]
    barrier = pltpu.get_barrier_semaphore()
    for peer in peers:
        pl.semaphore_signal(barrier, inc=1, device_id=peer, device_id_type=MESH)
    cp_ids.wait()
    ids_x[x] = jnp.concatenate([ids_in[...]] * nx, axis=1)
    cp_x.wait()
    for f in range(NC):
        xg[f][c, y, x] = x_in[:, pl.ds(OFFS[f], WIDTHS[f])]
    with scope("barrier"):
        pl.semaphore_wait(barrier, len(peers))

    def rc(src, dst, ss, rs, dev):
        return pltpu.make_async_remote_copy(
            src_ref=src, dst_ref=dst, send_sem=ss, recv_sem=rs, device_id=dev, device_id_type=MESH
        )

    def start(copies):
        for cp in copies:
            cp.start()

    def whole(ref, sems, at_):
        return rc(ref, ref, sems[0].at[*at_], sems[1].at[*at_], partner)

    gs = (g_s, g_r)

    def along_y(f):
        src = x_in.at[:, pl.ds(OFFS[f], WIDTHS[f])]
        return [
            rc(src, xg[f].at[c, y, x], g_s.at[f, 0], g_r.at[f, 0], at(x, ys[k], c)) for k in range(1, ny)
        ]

    def along_x(f):
        ref = xg[f].at[c, :, x]
        return [rc(ref, ref, g_s.at[f, 1], g_r.at[f, 1], at(xs[k], y, c)) for k in (1, nx - 1)]

    def relay(f):
        lo = xg[f].at[c, pl.ds(0, ny // 2), xs[nx - 1]]
        hi = xg[f].at[c, pl.ds(ny // 2, ny // 2), xs[1]]
        return [
            rc(lo, lo, g_s.at[f, 2], g_r.at[f, 2], at(xs[1], y, c)),
            rc(hi, hi, g_s.at[f, 2], g_r.at[f, 2], at(xs[nx - 1], y, c)),
        ]

    def across(f, k):
        ref = xg[f].at[c, :, xs[k]]
        return rc(ref, ref, g_s.at[f, 3], g_r.at[f, 3], partner)

    def all_of(f, step):
        ref = (
            xg[f].at[c, pl.ds(0, ny - 1), 0],
            xg[f].at[c, :, pl.ds(0, 2)],
            xg[f].at[c, :, 0],
            xg[f].at[c],
        )[step]
        return whole(ref, gs, (f, step))

    def gather1(f):
        start(along_y(f))

    def gather2(f):
        with scope(f"g2_{f}"):
            all_of(f, 0).wait_recv()
        start(along_x(f))
        across(f, 0).start()

    def gather3(f):
        with scope(f"g3_{f}"):
            all_of(f, 1).wait_recv()
        start(relay(f))
        across(f, 1).start()
        across(f, nx - 1).start()

    def gather4(f):
        with scope(f"g4_{f}"):
            all_of(f, 2).wait_recv()
        across(f, 2).start()

    def gather5(f):
        with scope(f"g5_{f}"):
            all_of(f, 3).wait_recv()

    id1 = [rc(ids_x.at[x], ids_x.at[x], id_s.at[0], id_r.at[0], at(xs[k], y, c)) for k in range(1, nx)]
    id2 = [rc(ids_g.at[c, y], ids_g.at[c, y], id_s.at[1], id_r.at[1], at(x, ys[k], c)) for k in range(1, ny)]
    id3 = rc(ids_g.at[c], ids_g.at[c], id_s.at[2], id_r.at[2], partner)
    id1_all = whole(ids_x.at[pl.ds(0, nx - 1)], (id_s, id_r), (0,))
    id2_all = whole(ids_g.at[c, pl.ds(0, ny - 1)], (id_s, id_r), (1,))

    blocks = [lax.rem(d + k, 8) for k in BLOCKS]
    kt = 2 * ny

    def build(g, core):
        lo, hi = GROUPS[g]

        def tile(k, _):
            ids = ids_g[core, k]
            t = core * ny + k
            low = ids & (ROWS - 1)
            block = ids >> 8
            word = low & 31
            bit = jnp.left_shift(1, (low >> 5) * 4)
            wide = lax.broadcasted_iota(jnp.int32, (32, 128), 0)
            vals = [jnp.where(block == blocks[i] * (2 * nx * ny) + v, bit, 0) for i in range(lo, hi)]
            acc = [[jnp.zeros((32, 128), jnp.int32) for _ in range(2)] for _ in vals]
            for j in range(LIST):
                eq = jnp.broadcast_to(word[j : j + 1], (32, 128)) == wide
                for n, val in enumerate(vals):
                    acc[n][j // 8] += jnp.where(eq, jnp.broadcast_to(val[j : j + 1], (32, 128)), 0)
            nib = 0x0F0F0F0F
            for n in range(len(vals)):
                a, b = acc[n]
                both = ((a & nib) + (b & nib), ((a >> 4) & nib) + ((b >> 4) & nib))
                for s in range(8):
                    count = (both[s % 2] >> (8 * (s // 2))) & 255
                    cnt[lo + n, pl.ds(32 * s, 32), pl.ds(pl.multiple_of(t * 128, 128), 128)] = count.astype(
                        jnp.float32
                    ).astype(jnp.bfloat16)
            return 0

        with scope(f"build{g}"):
            lax.fori_loop(0, ny, tile, 0)

    def dots(f, g):
        lo, hi = GROUPS[g]
        with scope(f"dot{f}{g}"):
            part[f][lo:hi] = jnp.dot(
                cnt[lo:hi].reshape((hi - lo) * ROWS, kt * 128),
                xg[f][...].reshape(kt * 128, WIDTHS[f]),
                preferred_element_type=jnp.float32,
            ).reshape(hi - lo, ROWS, WIDTHS[f])

    def zcopy(way, f, m):
        return rc(
            send[f].at[way, m], got[f].at[way, m], z_s.at[f], z_r.at[f, way, m], (down, up)[way]
        )

    def reduce(f, r):
        for m in ROUNDS[r]:
            for way in range(2):
                dist, half = MSG[m]
                half = half if way == 0 else 1 - half
                i = 0 if dist == 4 else 2 * (4 - dist) - 1 + way
                value = part[f][i, HALF * half : HALF * (half + 1)]
                if m >= 2:
                    with scope(f"w{f}{m - 2}"):
                        zcopy(way, f, m - 2).wait_recv()
                    value = value + got[f][way, m - 2].astype(jnp.float32)
                send[f][way, m] = value.astype(jnp.bfloat16)
                zcopy(way, f, m).start()

    def put(f):
        return pltpu.make_async_copy(outs[f], out_hbm.at[:, pl.ds(OFFS[f], WIDTHS[f])], out_sem.at[f])

    def finish(f):
        with scope(f"fin{f}"):
            for m in (5, 6):
                for way in range(2):
                    zcopy(way, f, m).wait_recv()
        for half in range(2):
            rows = slice(HALF * half, HALF * (half + 1))
            total = part[f][7, rows] + (
                got[f][0, 6 - half].astype(jnp.float32) + got[f][1, 5 + half].astype(jnp.float32)
            )
            outs[f][rows] = total * (1.0 / LIST)
        put(f).start()

    start(id1)
    gather1(0)
    with scope("id1"):
        id1_all.wait_recv()
    lane = lax.broadcasted_iota(jnp.int32, (LIST, 128), 1) // POS
    both = ids_x[0]
    for k in range(1, nx):
        both = jnp.where(lane == k, ids_x[k], both)
    ids_g[c, y] = both
    start(id2)
    gather1(1)
    gather2(0)
    with scope("id2"):
        id2_all.wait_recv()
    id3.start()
    build(0, c)
    gather3(0)
    with scope("id3"):
        id3.wait_recv()
    build(0, 1 - c)
    gather2(1)
    gather1(2)
    build(1, c)
    gather4(0)
    build(1, 1 - c)
    gather5(0)
    dots(0, 0)
    reduce(0, 0)
    gather3(1)
    dots(0, 1)
    build(2, c)
    gather2(2)
    gather1(3)
    build(2, 1 - c)
    gather4(1)
    reduce(0, 1)
    gather5(1)
    dots(1, 0)
    reduce(1, 0)
    gather3(2)
    dots(0, 2)
    reduce(0, 2)
    dots(1, 3)
    gather4(2)
    gather2(3)
    gather1(4)
    reduce(1, 1)
    gather5(2)
    dots(2, 0)
    reduce(2, 0)
    reduce(0, 3)
    dots(2, 3)
    gather3(3)
    reduce(1, 2)
    reduce(2, 1)
    gather2(4)
    finish(0)
    gather4(3)
    gather5(3)
    dots(3, 0)
    reduce(3, 0)
    reduce(1, 3)
    dots(3, 3)
    reduce(2, 2)
    gather3(4)
    reduce(3, 1)
    finish(1)
    gather4(4)
    gather5(4)
    dots(4, 4)
    reduce(4, 0)
    reduce(2, 3)
    reduce(3, 2)
    reduce(4, 1)
    finish(2)
    reduce(3, 3)
    reduce(4, 2)
    finish(3)
    reduce(4, 3)
    finish(4)

    with scope("drain"):
        id1_all.wait_send()
        id2_all.wait_send()
        id3.wait_send()
        for f in range(NC):
            for step in range(4):
                all_of(f, step).wait_send()
            rc(send[f], send[f], z_s.at[f], z_r.at[f, 0, 0], down).wait_send()
            put(f).wait()


def local(nx, ny, pooled_grad, token_ids):
    width = pooled_grad.shape[1]
    dma = pltpu.SemaphoreType.DMA
    bf = jnp.bfloat16
    vmem = pltpu.VMEM
    return pl.pallas_call(
        functools.partial(kernel, nx, ny),
        out_shape=jax.ShapeDtypeStruct((ROWS, width), jnp.float32),
        in_specs=[pl.BlockSpec(memory_space=pl.ANY)] * 2,
        out_specs=pl.BlockSpec(memory_space=pl.ANY),
        scratch_shapes=[
            vmem((POS, width), bf),
            vmem((LIST, POS), jnp.int32),
            vmem((nx, LIST, 128), jnp.int32),
            vmem((2, ny, LIST, 128), jnp.int32),
            vmem((8, ROWS, 2 * ny * 128), bf),
            *[vmem((2, ny, nx, POS, w), bf) for w in WIDTHS],
            *[vmem((8, ROWS, w), jnp.float32) for w in WIDTHS],
            *[vmem((2, 7, HALF, w), bf) for w in WIDTHS],
            *[vmem((2, 7, HALF, w), bf) for w in WIDTHS],
            *[vmem((ROWS, w), jnp.float32) for w in WIDTHS],
            dma((2,)), dma((NC,)), dma((3,)), dma((3,)),
            dma((NC, 4)), dma((NC, 4)), dma((NC,)), dma((NC, 2, 7)),
        ],
        compiler_params=pltpu.CompilerParams(
            collective_id=0, has_side_effects=True, vmem_limit_bytes=62 * 1024 * 1024
        ),
    )(pooled_grad, token_ids.T)


def solution(mesh, nx=4, ny=8):
    in_specs = (P(("dp", "vocab"), None), P(("dp", "vocab"), None))
    out_specs = P(("dp", "vocab"), None)
    return jax.shard_map(
        functools.partial(local, nx, ny), mesh=mesh, in_specs=in_specs, out_specs=out_specs, check_vma=False
    )
```

```python
import functools

import jax
import jax.numpy as jnp
from jax import lax
from jax.experimental import pallas as pl
from jax.experimental.pallas import tpu as pltpu
from jax.sharding import PartitionSpec as P

ROWS = 256
HALF = ROWS // 2
LIST = 16
POS = 32
WIDTHS = (128, 256, 256, 256, 128)
OFFS = tuple(sum(WIDTHS[:i]) for i in range(len(WIDTHS)))
NC = len(WIDTHS)
MESH = pl.DeviceIdType.MESH
MSG = ((4, 0), (3, 1), (3, 0), (2, 1), (2, 0), (1, 1), (1, 0))
ROUNDS = ((0, 1), (2, 3), (4, 5), (6,))
BLOCKS = (4, 5, 3, 6, 2, 7, 1, 0)
GROUPS = ((0, 3), (3, 5), (5, 8), (3, 8), (0, 8))


def kernel(nx, ny, x_hbm, ids_hbm, out_ref, x_in, ids_in, ids_x, ids_g, cnt, *rest):
    xg, part, send, got = (rest[NC * i : NC * (i + 1)] for i in range(4))
    in_sem, id_s, id_r, g_s, g_r, z_s, z_r = rest[4 * NC :]
    scope = jax.named_scope
    d = lax.axis_index("dp")
    v = lax.axis_index("vocab")
    c = v % 2
    y = (v // 2) % ny
    x = v // (2 * ny)

    def at(xx, yy, cc):
        return (d, (xx * ny + yy) * 2 + cc)

    xs = [lax.rem(x + k, nx) for k in range(nx)]
    ys = [lax.rem(y + k, ny) for k in range(ny)]
    partner = at(x, y, 1 - c)
    down = (lax.rem(d + 7, 8), v)
    up = (lax.rem(d + 1, 8), v)

    cp_ids = pltpu.make_async_copy(ids_hbm, ids_in, in_sem.at[0])
    cp_x = pltpu.make_async_copy(x_hbm, x_in, in_sem.at[1])
    cp_ids.start()
    cp_x.start()

    peers = [at(x, ys[k], c) for k in range(1, ny)] + [at(xs[k], y, c) for k in range(1, nx)]
    peers += [partner, down, up]
    barrier = pltpu.get_barrier_semaphore()
    for peer in peers:
        pl.semaphore_signal(barrier, inc=1, device_id=peer, device_id_type=MESH)
    cp_ids.wait()
    ids_x[x] = jnp.concatenate([ids_in[...]] * nx, axis=1)
    cp_x.wait()
    for f in range(NC):
        xg[f][c, y, x] = x_in[:, pl.ds(OFFS[f], WIDTHS[f])]
    with scope("barrier"):
        pl.semaphore_wait(barrier, len(peers))

    def rc(src, dst, ss, rs, dev):
        return pltpu.make_async_remote_copy(
            src_ref=src, dst_ref=dst, send_sem=ss, recv_sem=rs, device_id=dev, device_id_type=MESH
        )

    def start(copies):
        for cp in copies:
            cp.start()

    def whole(ref, i):
        return rc(ref, ref, id_s.at[i], id_r.at[i], partner)

    def along_y(f):
        src = x_in.at[:, pl.ds(OFFS[f], WIDTHS[f])]
        return [
            rc(src, xg[f].at[c, y, x], g_s.at[0], g_r.at[f, 0], at(x, ys[k], c)) for k in range(1, ny)
        ]

    def along_x(f):
        ref = xg[f].at[c, :, x]
        return [rc(ref, ref, g_s.at[1], g_r.at[f, 1], at(xs[k], y, c)) for k in (1, nx - 1)]

    def relay(f):
        lo = xg[f].at[c, pl.ds(0, ny // 2), xs[nx - 1]]
        hi = xg[f].at[c, pl.ds(ny // 2, ny // 2), xs[1]]
        return [
            rc(lo, lo, g_s.at[2], g_r.at[f, 2], at(xs[1], y, c)),
            rc(hi, hi, g_s.at[2], g_r.at[f, 2], at(xs[nx - 1], y, c)),
        ]

    def across(f, k):
        ref = xg[f].at[c, :, xs[k]]
        return rc(ref, ref, g_s.at[3], g_r.at[f, 3], partner)

    def all_of(f, step):
        ref = (
            xg[f].at[c, pl.ds(0, ny - 1), 0],
            xg[f].at[c, :, pl.ds(0, 2)],
            xg[f].at[c, :, 0],
            xg[f].at[c],
        )[step]
        return rc(ref, ref, g_s.at[step], g_r.at[f, step], partner)

    def gather1(f):
        start(along_y(f))

    def gather2(f):
        with scope(f"g2_{f}"):
            all_of(f, 0).wait_recv()
        start(along_x(f))
        across(f, 0).start()

    def gather3(f):
        with scope(f"g3_{f}"):
            all_of(f, 1).wait_recv()
        start(relay(f))
        across(f, 1).start()
        across(f, nx - 1).start()

    def gather4(f):
        with scope(f"g4_{f}"):
            all_of(f, 2).wait_recv()
        across(f, 2).start()

    def gather5(f):
        with scope(f"g5_{f}"):
            all_of(f, 3).wait_recv()

    id1 = [rc(ids_x.at[x], ids_x.at[x], id_s.at[0], id_r.at[0], at(xs[k], y, c)) for k in range(1, nx)]
    id2 = [rc(ids_g.at[c, y], ids_g.at[c, y], id_s.at[1], id_r.at[1], at(x, ys[k], c)) for k in range(1, ny)]
    id3 = rc(ids_g.at[c], ids_g.at[c], id_s.at[2], id_r.at[2], partner)
    id1_all = whole(ids_x.at[pl.ds(0, nx - 1)], 0)
    id2_all = whole(ids_g.at[c, pl.ds(0, ny - 1)], 1)

    blocks = [lax.rem(d + k, 8) for k in BLOCKS]
    kt = 2 * ny

    def build(g, core):
        lo, hi = GROUPS[g]

        def tile(k, _):
            ids = ids_g[core, k]
            t = core * ny + k
            low = ids & (ROWS - 1)
            block = ids >> 8
            word = low & 31
            bit = jnp.left_shift(1, (low >> 5) * 4)
            wide = lax.broadcasted_iota(jnp.int32, (32, 128), 0)
            vals = [jnp.where(block == blocks[i] * (2 * nx * ny) + v, bit, 0) for i in range(lo, hi)]
            acc = [[jnp.zeros((32, 128), jnp.int32) for _ in range(2)] for _ in vals]
            for j in range(LIST):
                eq = jnp.broadcast_to(word[j : j + 1], (32, 128)) == wide
                for n, val in enumerate(vals):
                    acc[n][j // 8] += jnp.where(eq, jnp.broadcast_to(val[j : j + 1], (32, 128)), 0)
            nib = 0x0F0F0F0F
            for n in range(len(vals)):
                a, b = acc[n]
                both = ((a & nib) + (b & nib), ((a >> 4) & nib) + ((b >> 4) & nib))
                for s in range(8):
                    count = (both[s % 2] >> (8 * (s // 2))) & 255
                    cnt[pl.ds(ROWS * (lo + n) + 32 * s, 32), pl.ds(pl.multiple_of(t * 128, 128), 128)] = count.astype(
                        jnp.float32
                    ).astype(jnp.bfloat16)
            return 0

        with scope(f"build{g}"):
            lax.fori_loop(0, ny, tile, 0)

    once = jnp.minimum(d + 1, 1)

    def dots(f, g):
        lo, hi = GROUPS[g]

        def body(_, carry):
            part[f][lo:hi] = jnp.dot(
                cnt[ROWS * lo : ROWS * hi],
                xg[f][...].reshape(kt * 128, WIDTHS[f]),
                preferred_element_type=jnp.float32,
            ).reshape(hi - lo, ROWS, WIDTHS[f])
            return carry

        with scope(f"dot{f}{g}"):
            lax.fori_loop(0, once, body, 0)

    def zcopy(way, f, m):
        return rc(
            send[f].at[way, m], got[f].at[way, m], z_s.at[0], z_r.at[f, way, m], (down, up)[way]
        )

    def reduce(f, r):
        for m in ROUNDS[r]:
            for way in range(2):
                dist, half = MSG[m]
                half = half if way == 0 else 1 - half
                i = 0 if dist == 4 else 2 * (4 - dist) - 1 + way
                value = part[f][i, HALF * half : HALF * (half + 1)]
                if m >= 2:
                    with scope(f"w{f}{m - 2}"):
                        zcopy(way, f, m - 2).wait_recv()
                    value = value + got[f][way, m - 2].astype(jnp.float32)
                send[f][way, m] = value.astype(jnp.bfloat16)
                zcopy(way, f, m).start()

    def finish(f):
        with scope(f"fin{f}"):
            for m in (5, 6):
                for way in range(2):
                    zcopy(way, f, m).wait_recv()
        for half in range(2):
            rows = slice(HALF * half, HALF * (half + 1))
            total = part[f][7, rows] + (
                got[f][0, 6 - half].astype(jnp.float32) + got[f][1, 5 + half].astype(jnp.float32)
            )
            out_ref[rows, OFFS[f] : OFFS[f] + WIDTHS[f]] = total * (1.0 / LIST)

    start(id1)
    gather1(0)
    gather1(1)
    with scope("id1"):
        id1_all.wait_recv()
    lane = lax.broadcasted_iota(jnp.int32, (LIST, 128), 1) // POS
    both = ids_x[0]
    for k in range(1, nx):
        both = jnp.where(lane == k, ids_x[k], both)
    ids_g[c, y] = both
    start(id2)
    gather1(2)
    gather2(0)
    gather2(1)
    with scope("id2"):
        id2_all.wait_recv()
    id3.start()
    gather3(0)
    build(0, c)
    with scope("id3"):
        id3.wait_recv()
    build(0, 1 - c)
    gather3(1)
    gather2(2)
    gather1(3)
    gather1(4)
    build(1, c)
    gather4(0)
    build(1, 1 - c)
    gather5(0)
    dots(0, 0)
    reduce(0, 0)
    build(2, c)
    dots(0, 1)
    gather4(1)
    gather5(1)
    dots(1, 0)
    reduce(0, 1)
    reduce(1, 0)
    gather3(2)
    gather2(3)
    build(2, 1 - c)
    dots(0, 2)
    dots(1, 3)
    reduce(0, 2)
    gather4(2)
    reduce(1, 1)
    gather3(3)
    gather2(4)
    gather5(2)
    dots(2, 0)
    reduce(2, 0)
    reduce(0, 3)
    dots(2, 3)
    reduce(1, 2)
    gather3(4)
    gather4(3)
    reduce(2, 1)
    gather5(3)
    dots(3, 4)
    reduce(3, 0)
    gather4(4)
    gather5(4)
    dots(4, 4)
    reduce(4, 0)
    finish(0)
    reduce(1, 3)
    reduce(2, 2)
    reduce(3, 1)
    reduce(4, 1)
    finish(1)
    reduce(2, 3)
    reduce(3, 2)
    reduce(4, 2)
    finish(2)
    reduce(3, 3)
    reduce(4, 3)
    finish(3)
    finish(4)

    with scope("drain"):
        id1_all.wait_send()
        id2_all.wait_send()
        id3.wait_send()
        width = x_in.shape[1]
        depth = kt * 128
        for step, rows in enumerate(((ny - 1) * POS, 2 * ny * POS, ny * POS, nx * ny * POS)):
            ref = cnt.at[pl.ds(0, rows * width // depth)]
            rc(ref, ref, g_s.at[step], g_r.at[0, step], partner).wait_send()
        ref = cnt.at[pl.ds(0, 14 * HALF * width // depth)]
        rc(ref, ref, z_s.at[0], z_r.at[0, 0, 0], down).wait_send()


def local(nx, ny, pooled_grad, token_ids):
    width = pooled_grad.shape[1]
    dma = pltpu.SemaphoreType.DMA
    bf = jnp.bfloat16
    vmem = pltpu.VMEM
    return pl.pallas_call(
        functools.partial(kernel, nx, ny),
        out_shape=jax.ShapeDtypeStruct((ROWS, width), jnp.float32),
        in_specs=[pl.BlockSpec(memory_space=pl.ANY)] * 2,
        out_specs=pl.BlockSpec(memory_space=pltpu.VMEM),
        scratch_shapes=[
            vmem((POS, width), bf),
            vmem((LIST, POS), jnp.int32),
            vmem((nx, LIST, 128), jnp.int32),
            vmem((2, ny, LIST, 128), jnp.int32),
            vmem((8 * ROWS, 2 * ny * 128), bf),
            *[vmem((2, ny, nx, POS, w), bf) for w in WIDTHS],
            *[vmem((8, ROWS, w), jnp.float32) for w in WIDTHS],
            *[vmem((2, 7, HALF, w), bf) for w in WIDTHS],
            *[vmem((2, 7, HALF, w), bf) for w in WIDTHS],
            dma((2,)), dma((3,)), dma((3,)),
            dma((4,)), dma((NC, 4)), dma((1,)), dma((NC, 2, 7)),
        ],
        compiler_params=pltpu.CompilerParams(
            collective_id=0, has_side_effects=True, vmem_limit_bytes=62 * 1024 * 1024
        ),
    )(pooled_grad, token_ids.T)


def solution(mesh, nx=4, ny=8):
    in_specs = (P(("dp", "vocab"), None), P(("dp", "vocab"), None))
    out_specs = P(("dp", "vocab"), None)
    return jax.shard_map(
        functools.partial(local, nx, ny), mesh=mesh, in_specs=in_specs, out_specs=out_specs, check_vma=False
    )
```

```python
import functools

import jax
import jax.numpy as jnp
from jax import lax
from jax.experimental import pallas as pl
from jax.experimental.pallas import tpu as pltpu
from jax.sharding import PartitionSpec as P

ROWS = 256
HALF = ROWS // 2
LIST = 16
POS = 32
WIDTHS = (128, 256, 256, 256, 128)
OFFS = tuple(sum(WIDTHS[:i]) for i in range(len(WIDTHS)))
NC = len(WIDTHS)
MESH = pl.DeviceIdType.MESH
MSG = ((3, 0), (3, 1), (2, 0), (2, 1), (1, 0), (1, 1))
ROUNDS = ((0, 1), (2, 3), (4, 5))
BLOCKS = (0, 5, 3, 6, 2, 7, 1, 0)
FAR, A, B, C, BC, ABC = (0, 1), (1, 3), (3, 5), (5, 8), (3, 8), (1, 8)


def kernel(nx, ny, x_hbm, ids_hbm, out_ref, x_in, x_far, ids_in, ids_far, ids_x, ids_g, cnt, *rest):
    part, send, got = (rest[NC * i : NC * (i + 1)] for i in range(3))
    xg = rest[3 * NC : 5 * NC]
    in_sem, id_s, id_r, g_s, g_r, z_s, z_r = rest[5 * NC :]
    scope = jax.named_scope
    d = lax.axis_index("dp")
    v = lax.axis_index("vocab")
    c = v % 2
    y = (v // 2) % ny
    x = v // (2 * ny)

    def at(xx, yy, cc):
        return (d, (xx * ny + yy) * 2 + cc)

    far_first = [sorted(range(1, n), key=lambda k, n=n: -min(k, n - k)) for n in (nx, ny)]
    xs = [lax.rem(x + k, nx) for k in range(nx)]
    ys = [lax.rem(y + k, ny) for k in range(ny)]
    partner = at(x, y, 1 - c)
    down = (lax.rem(d + 7, 8), v)
    up = (lax.rem(d + 1, 8), v)
    far = (lax.rem(d + 4, 8), v)

    cp_ids = pltpu.make_async_copy(ids_hbm, ids_in, in_sem.at[0])
    cp_x = pltpu.make_async_copy(x_hbm, x_in, in_sem.at[1])
    cp_ids.start()
    cp_x.start()

    peers = [at(x, ys[k], c) for k in range(1, ny)] + [at(xs[k], y, c) for k in range(1, nx)]
    peers += [partner, down, up, far]
    barrier = pltpu.get_barrier_semaphore()
    for peer in peers:
        pl.semaphore_signal(barrier, inc=1, device_id=peer, device_id_type=MESH)
    cp_ids.wait()
    ids_x[0, x] = jnp.concatenate([ids_in[...]] * nx, axis=1)
    cp_x.wait()
    for f in range(NC):
        xg[f][c, y, x] = x_in[:, pl.ds(OFFS[f], WIDTHS[f])]
    with scope("barrier"):
        pl.semaphore_wait(barrier, len(peers))

    def rc(src, dst, ss, rs, dev):
        return pltpu.make_async_remote_copy(
            src_ref=src, dst_ref=dst, send_sem=ss, recv_sem=rs, device_id=dev, device_id_type=MESH
        )

    def start(copies):
        for cp in copies:
            cp.start()

    def whole(ref, i):
        return rc(ref, ref, id_s.at[i], id_r.at[i], partner)

    def along_y(f):
        src = (x_in if f < NC else x_far).at[:, pl.ds(OFFS[f % NC], WIDTHS[f % NC])]
        return [
            rc(src, xg[f].at[c, y, x], g_s.at[0], g_r.at[f, 0], at(x, ys[k], c)) for k in far_first[1]
        ]

    def along_x(f):
        ref = xg[f].at[c, :, x]
        return [rc(ref, ref, g_s.at[1], g_r.at[f, 1], at(xs[k], y, c)) for k in (1, nx - 1)]

    def relay(f):
        lo = xg[f].at[c, pl.ds(0, ny // 2), xs[nx - 1]]
        hi = xg[f].at[c, pl.ds(ny // 2, ny // 2), xs[1]]
        return [
            rc(lo, lo, g_s.at[2], g_r.at[f, 2], at(xs[1], y, c)),
            rc(hi, hi, g_s.at[2], g_r.at[f, 2], at(xs[nx - 1], y, c)),
        ]

    def across(f, k):
        ref = xg[f].at[c, :, xs[k]]
        return rc(ref, ref, g_s.at[3], g_r.at[f, 3], partner)

    def all_of(f, step):
        ref = (
            xg[f].at[c, pl.ds(0, ny - 1), 0],
            xg[f].at[c, :, pl.ds(0, 2)],
            xg[f].at[c, :, 0],
            xg[f].at[c],
        )[step]
        return rc(ref, ref, g_s.at[step], g_r.at[f, step], partner)

    def gather1(f):
        start(along_y(f))

    def gather2(f):
        with scope(f"g2_{f}"):
            all_of(f, 0).wait_recv()
        start(along_x(f))
        across(f, 0).start()

    def gather3(f):
        with scope(f"g3_{f}"):
            all_of(f, 1).wait_recv()
        start(relay(f))
        across(f, 1).start()
        across(f, nx - 1).start()

    def gather4(f):
        with scope(f"g4_{f}"):
            all_of(f, 2).wait_recv()
        across(f, 2).start()

    def gather5(f):
        with scope(f"g5_{f}"):
            all_of(f, 3).wait_recv()

    def ids_copies(e):
        near = ids_x.at[e, x]
        line = ids_g.at[e, c, y]
        plane = ids_g.at[e, c]
        k = 3 * e
        return (
            [rc(near, near, id_s.at[k], id_r.at[k], at(xs[i], y, c)) for i in far_first[0]],
            [rc(line, line, id_s.at[k + 1], id_r.at[k + 1], at(x, ys[i], c)) for i in far_first[1]],
            [rc(plane, plane, id_s.at[k + 2], id_r.at[k + 2], partner)],
            whole(ids_x.at[e, pl.ds(0, nx - 1)], k),
            whole(ids_g.at[e, c, pl.ds(0, ny - 1)], k + 1),
            whole(plane, k + 2),
        )

    ids_near, ids_away = ids_copies(0), ids_copies(1)

    def join(e):
        lane = lax.broadcasted_iota(jnp.int32, (LIST, 128), 1) // POS
        both = ids_x[e, 0]
        for k in range(1, nx):
            both = jnp.where(lane == k, ids_x[e, k], both)
        ids_g[e, c, y] = both

    to_far = (
        rc(ids_x.at[0, x], ids_far, id_s.at[6], id_r.at[6], far),
        rc(x_in, x_far, id_s.at[7], id_r.at[7], far),
    )

    blocks = [lax.rem(d + k, 8) for k in BLOCKS]
    kt = 2 * ny

    def build(g, core, e=0):
        lo, hi = g

        def tile(k, _):
            ids = ids_g[e, core, k]
            t = core * ny + k
            low = ids & (ROWS - 1)
            block = ids >> 8
            word = low & 31
            bit = jnp.left_shift(1, (low >> 5) * 4)
            wide = lax.broadcasted_iota(jnp.int32, (32, 128), 0)
            vals = [jnp.where(block == blocks[i] * (2 * nx * ny) + v, bit, 0) for i in range(lo, hi)]
            acc = [[jnp.zeros((32, 128), jnp.int32) for _ in range(2)] for _ in vals]
            for j in range(LIST):
                eq = jnp.broadcast_to(word[j : j + 1], (32, 128)) == wide
                for n, val in enumerate(vals):
                    acc[n][j // 8] += jnp.where(eq, jnp.broadcast_to(val[j : j + 1], (32, 128)), 0)
            nib = 0x0F0F0F0F
            for n in range(len(vals)):
                a, b = acc[n]
                both = ((a & nib) + (b & nib), ((a >> 4) & nib) + ((b >> 4) & nib))
                for s in range(8):
                    count = (both[s % 2] >> (8 * (s // 2))) & 255
                    cnt[pl.ds(ROWS * (lo + n) + 32 * s, 32), pl.ds(pl.multiple_of(t * 128, 128), 128)] = count.astype(
                        jnp.float32
                    ).astype(jnp.bfloat16)
            return 0

        with scope(f"build{lo}"):
            lax.fori_loop(0, ny, tile, 0)

    once = jnp.minimum(d + 1, 1)

    def dots(f, g):
        lo, hi = g
        rows = xg[f + NC] if g is FAR else xg[f]

        def body(_, carry):
            part[f][lo:hi] = jnp.dot(
                cnt[ROWS * lo : ROWS * hi],
                rows[...].reshape(kt * 128, WIDTHS[f]),
                preferred_element_type=jnp.float32,
            ).reshape(hi - lo, ROWS, WIDTHS[f])
            return carry

        with scope(f"dot{f}{lo}"):
            lax.fori_loop(0, once, body, 0)

    def zcopy(way, f, m):
        return rc(
            send[f].at[way, m], got[f].at[way, m], z_s.at[0], z_r.at[f, m], (down, up)[way]
        )

    def zwait(f, m):
        ref = got[f].at[:, m]
        with scope(f"w{f}{m}"):
            rc(ref, ref, z_s.at[0], z_r.at[f, m], down).wait_recv()

    def reduce(f, r, some=(0, 1)):
        for m in (ROUNDS[r][i] for i in some):
            dist, half = MSG[m]
            if m >= 2:
                zwait(f, m - 2)
            for way in range(2):
                i = 2 * (4 - dist) - 1 + way
                value = part[f][i, HALF * half : HALF * (half + 1)]
                if m >= 2:
                    value = value + got[f][way, m - 2].astype(jnp.float32)
                send[f][way, m] = value.astype(jnp.bfloat16)
                zcopy(way, f, m).start()

    def finish(f):
        gather5(f + NC)
        dots(f, FAR)
        for half in range(2):
            zwait(f, 4 + half)
            rows = slice(HALF * half, HALF * (half + 1))
            total = (part[f][7, rows] + part[f][0, rows]) + (
                got[f][0, 4 + half].astype(jnp.float32) + got[f][1, 4 + half].astype(jnp.float32)
            )
            out_ref[rows, OFFS[f] : OFFS[f] + WIDTHS[f]] = total * (1.0 / LIST)

    start(ids_near[0])
    gather1(0)
    gather1(1)
    start(to_far)
    with scope("id1"):
        ids_near[3].wait_recv()
    join(0)
    start(ids_near[1])
    gather1(2)
    gather2(0)
    gather2(1)
    with scope("id2"):
        ids_near[4].wait_recv()
    start(ids_near[2])
    gather3(0)
    build(A, c)
    with scope("id3"):
        ids_near[5].wait_recv()
    build(A, 1 - c)
    gather3(1)
    gather2(2)
    gather1(3)
    gather1(4)
    to_far[0].wait_recv()
    ids_x[1, x] = ids_far[...]
    start(ids_away[0])
    build(B, c)
    gather4(0)
    build(B, 1 - c)
    gather5(0)
    dots(0, A)
    reduce(0, 0)
    to_far[1].wait_recv()
    for f in range(NC):
        xg[NC + f][c, y, x] = x_far[:, pl.ds(OFFS[f], WIDTHS[f])]
        gather1(NC + f)
    build(C, c)
    dots(0, B)
    gather4(1)
    gather5(1)
    dots(1, A)
    reduce(0, 1)
    reduce(1, 0)
    gather3(2)
    gather2(3)
    with scope("far"):
        ids_away[3].wait_recv()
    join(1)
    start(ids_away[1])
    build(C, 1 - c)
    dots(0, C)
    dots(1, BC)
    reduce(0, 2)
    gather4(2)
    reduce(1, 1)
    gather3(3)
    gather2(4)
    gather2(5)
    gather5(2)
    dots(2, A)
    reduce(2, 0)
    dots(2, BC)
    with scope("id2far"):
        ids_away[4].wait_recv()
    start(ids_away[2])
    reduce(1, 2)
    gather3(4)
    gather4(3)
    gather2(6)
    gather3(5)
    reduce(2, 1)
    gather2(7)
    gather5(3)
    dots(3, ABC)
    reduce(3, 0)
    gather4(4)
    gather5(4)
    gather2(8)
    dots(4, ABC)
    reduce(4, 0)
    gather4(5)
    gather3(6)
    gather2(9)
    reduce(2, 2)
    ids_away[5].wait_recv()
    build(FAR, c, 1)
    build(FAR, 1 - c, 1)
    gather3(7)
    reduce(3, 1)
    reduce(4, 1)
    finish(0)
    gather4(6)
    gather3(8)
    reduce(3, 2, (0,))
    gather4(7)
    gather3(9)
    reduce(3, 2, (1,))
    finish(1)
    reduce(4, 2)
    gather4(8)
    finish(2)
    gather4(9)
    finish(3)
    finish(4)

    with scope("drain"):
        for copies in (ids_near, ids_away):
            for step in (3, 4, 5):
                copies[step].wait_send()
        for cp in to_far:
            cp.wait_send()
        width = x_in.shape[1]
        depth = kt * 128
        for step, rows in enumerate(((ny - 1) * POS, 2 * ny * POS, ny * POS, nx * ny * POS)):
            ref = cnt.at[pl.ds(0, 2 * rows * width // depth)]
            rc(ref, ref, g_s.at[step], g_r.at[0, step], partner).wait_send()
        ref = cnt.at[pl.ds(0, 2 * len(MSG) * HALF * width // depth)]
        rc(ref, ref, z_s.at[0], z_r.at[0, 0], down).wait_send()


def local(nx, ny, pooled_grad, token_ids):
    width = pooled_grad.shape[1]
    dma = pltpu.SemaphoreType.DMA
    bf = jnp.bfloat16
    vmem = pltpu.VMEM
    return pl.pallas_call(
        functools.partial(kernel, nx, ny),
        out_shape=jax.ShapeDtypeStruct((ROWS, width), jnp.float32),
        in_specs=[pl.BlockSpec(memory_space=pl.ANY)] * 2,
        out_specs=pl.BlockSpec(memory_space=pltpu.VMEM),
        scratch_shapes=[
            vmem((POS, width), bf),
            vmem((POS, width), bf),
            vmem((LIST, POS), jnp.int32),
            vmem((LIST, 128), jnp.int32),
            vmem((2, nx, LIST, 128), jnp.int32),
            vmem((2, 2, ny, LIST, 128), jnp.int32),
            vmem((8 * ROWS, 2 * ny * 128), bf),
            *[vmem((8, ROWS, w), jnp.float32) for w in WIDTHS],
            *[vmem((2, len(MSG), HALF, w), bf) for w in WIDTHS],
            *[vmem((2, len(MSG), HALF, w), bf) for w in WIDTHS],
            *[vmem((2, ny, nx, POS, w), bf) for w in WIDTHS + WIDTHS],
            dma((2,)), dma((8,)), dma((8,)),
            dma((4,)), dma((2 * NC, 4)), dma((1,)), dma((NC, len(MSG))),
        ],
        compiler_params=pltpu.CompilerParams(
            collective_id=0, has_side_effects=True, vmem_limit_bytes=62 * 1024 * 1024
        ),
    )(pooled_grad, token_ids.T)


def solution(mesh, nx=4, ny=8):
    in_specs = (P(("dp", "vocab"), None), P(("dp", "vocab"), None))
    out_specs = P(("dp", "vocab"), None)
    return jax.shard_map(
        functools.partial(local, nx, ny), mesh=mesh, in_specs=in_specs, out_specs=out_specs, check_vma=False
    )
```

```python
import functools

import jax
import jax.numpy as jnp
from jax import lax
from jax.experimental import pallas as pl
from jax.experimental.pallas import tpu as pltpu
from jax.sharding import PartitionSpec as P

ROWS = 256
HALF = ROWS // 2
LIST = 16
POS = 32
WIDTHS = (128, 256, 256, 256, 128)
OFFS = tuple(sum(WIDTHS[:i]) for i in range(len(WIDTHS)))
NC = len(WIDTHS)
MESH = pl.DeviceIdType.MESH
MSG = ((3, 0), (3, 1), (2, 0), (2, 1), (1, 0), (1, 1))
ROUNDS = ((0, 1), (2, 3), (4, 5))
BLOCKS = (0, 5, 3, 6, 2, 7, 1, 0)
FAR, A, B, C, BC, ABC = (0, 1), (1, 3), (3, 5), (5, 8), (3, 8), (1, 8)


def kernel(nx, ny, x_hbm, ids_hbm, out_ref, x_in, x_far, ids_in, ids_far, ids_x, ids_g, cnt, *rest):
    part, send, got = (rest[NC * i : NC * (i + 1)] for i in range(3))
    xg = rest[3 * NC : 5 * NC]
    in_sem, id_s, id_r, g_s, g_r, z_s, z_r = rest[5 * NC :]
    scope = jax.named_scope
    d = lax.axis_index("dp")
    v = lax.axis_index("vocab")
    c = v % 2
    y = (v // 2) % ny
    x = v // (2 * ny)

    def at(xx, yy, cc):
        return (d, (xx * ny + yy) * 2 + cc)

    far_first = [sorted(range(1, n), key=lambda k, n=n: -min(k, n - k)) for n in (nx, ny)]
    xs = [lax.rem(x + k, nx) for k in range(nx)]
    ys = [lax.rem(y + k, ny) for k in range(ny)]
    partner = at(x, y, 1 - c)
    down = (lax.rem(d + 7, 8), v)
    up = (lax.rem(d + 1, 8), v)
    far = (lax.rem(d + 4, 8), v)

    cp_ids = pltpu.make_async_copy(ids_hbm, ids_in, in_sem.at[0])
    cp_x = pltpu.make_async_copy(x_hbm, x_in, in_sem.at[1])
    cp_ids.start()
    cp_x.start()

    peers = [at(x, ys[k], c) for k in range(1, ny)] + [at(xs[k], y, c) for k in range(1, nx)]
    peers += [partner, down, up, far]
    barrier = pltpu.get_barrier_semaphore()
    for peer in peers:
        pl.semaphore_signal(barrier, inc=1, device_id=peer, device_id_type=MESH)
    cp_ids.wait()
    ids_x[0, x] = jnp.concatenate([ids_in[...]] * nx, axis=1)
    cp_x.wait()
    for f in range(NC):
        xg[f][c, y, x] = x_in[:, pl.ds(OFFS[f], WIDTHS[f])]
    with scope("barrier"):
        pl.semaphore_wait(barrier, len(peers))

    def rc(src, dst, ss, rs, dev):
        return pltpu.make_async_remote_copy(
            src_ref=src, dst_ref=dst, send_sem=ss, recv_sem=rs, device_id=dev, device_id_type=MESH
        )

    def start(copies):
        for cp in copies:
            cp.start()

    def whole(ref, i):
        return rc(ref, ref, id_s.at[i], id_r.at[i], partner)

    def along_y(f):
        src = (x_in if f < NC else x_far).at[:, pl.ds(OFFS[f % NC], WIDTHS[f % NC])]
        return [
            rc(src, xg[f].at[c, y, x], g_s.at[0], g_r.at[f, 0], at(x, ys[k], c)) for k in far_first[1]
        ]

    def along_x(f):
        ref = xg[f].at[c, :, x]
        return [rc(ref, ref, g_s.at[1], g_r.at[f, 1], at(xs[k], y, c)) for k in (1, nx - 1)]

    def relay(f):
        lo = xg[f].at[c, pl.ds(0, ny // 2), xs[nx - 1]]
        hi = xg[f].at[c, pl.ds(ny // 2, ny // 2), xs[1]]
        return [
            rc(lo, lo, g_s.at[2], g_r.at[f, 2], at(xs[1], y, c)),
            rc(hi, hi, g_s.at[2], g_r.at[f, 2], at(xs[nx - 1], y, c)),
        ]

    def across(f, k):
        ref = xg[f].at[c, :, xs[k]]
        return rc(ref, ref, g_s.at[3], g_r.at[f, 3], partner)

    def all_of(f, step):
        ref = (
            xg[f].at[c, pl.ds(0, ny - 1), 0],
            xg[f].at[c, :, pl.ds(0, 2)],
            xg[f].at[c, :, 0],
            xg[f].at[c],
        )[step]
        return rc(ref, ref, g_s.at[step], g_r.at[f, step], partner)

    def gather1(f):
        start(along_y(f))

    def gather2(f):
        with scope(f"g2_{f}"):
            all_of(f, 0).wait_recv()
        start(along_x(f))
        across(f, 0).start()

    def gather3(f):
        with scope(f"g3_{f}"):
            all_of(f, 1).wait_recv()
        start(relay(f))
        across(f, 1).start()
        across(f, nx - 1).start()

    def gather4(f):
        with scope(f"g4_{f}"):
            all_of(f, 2).wait_recv()
        across(f, 2).start()

    def gather5(f):
        with scope(f"g5_{f}"):
            all_of(f, 3).wait_recv()

    def ids_copies(e):
        near = ids_x.at[e, x]
        line = ids_g.at[e, c, y]
        plane = ids_g.at[e, c]
        k = 3 * e
        return (
            [rc(near, near, id_s.at[k], id_r.at[k], at(xs[i], y, c)) for i in far_first[0]],
            [rc(line, line, id_s.at[k + 1], id_r.at[k + 1], at(x, ys[i], c)) for i in far_first[1]],
            [rc(plane, plane, id_s.at[k + 2], id_r.at[k + 2], partner)],
            whole(ids_x.at[e, pl.ds(0, nx - 1)], k),
            whole(ids_g.at[e, c, pl.ds(0, ny - 1)], k + 1),
            whole(plane, k + 2),
        )

    ids_near, ids_away = ids_copies(0), ids_copies(1)

    def join(e):
        lane = lax.broadcasted_iota(jnp.int32, (LIST, 128), 1) // POS
        both = ids_x[e, 0]
        for k in range(1, nx):
            both = jnp.where(lane == k, ids_x[e, k], both)
        ids_g[e, c, y] = both

    to_far = (
        rc(ids_x.at[0, x], ids_far, id_s.at[6], id_r.at[6], far),
        rc(x_in, x_far, id_s.at[7], id_r.at[7], far),
    )

    blocks = [lax.rem(d + k, 8) for k in BLOCKS]
    kt = 2 * ny

    def build(g, core, e=0):
        lo, hi = g

        def tile(k, _):
            ids = ids_g[e, core, k]
            t = core * ny + k
            low = ids & (ROWS - 1)
            block = ids >> 8
            word = low & 31
            bit = jnp.left_shift(1, (low >> 5) * 4)
            wide = lax.broadcasted_iota(jnp.int32, (32, 128), 0)
            vals = [jnp.where(block == blocks[i] * (2 * nx * ny) + v, bit, 0) for i in range(lo, hi)]
            acc = [[jnp.zeros((32, 128), jnp.int32) for _ in range(2)] for _ in vals]
            for j in range(LIST):
                eq = jnp.broadcast_to(word[j : j + 1], (32, 128)) == wide
                for n, val in enumerate(vals):
                    acc[n][j // 8] += jnp.where(eq, jnp.broadcast_to(val[j : j + 1], (32, 128)), 0)
            nib = 0x0F0F0F0F
            for n in range(len(vals)):
                a, b = acc[n]
                both = ((a & nib) + (b & nib), ((a >> 4) & nib) + ((b >> 4) & nib))
                for s in range(8):
                    count = (both[s % 2] >> (8 * (s // 2))) & 255
                    cnt[pl.ds(ROWS * (lo + n) + 32 * s, 32), pl.ds(pl.multiple_of(t * 128, 128), 128)] = count.astype(
                        jnp.float32
                    ).astype(jnp.bfloat16)
            return 0

        with scope(f"build{lo}"):
            lax.fori_loop(0, ny, tile, 0)

    once = jnp.minimum(d + 1, 1)

    def dots(f, g):
        lo, hi = g
        rows = xg[f + NC] if g is FAR else xg[f]

        def body(_, carry):
            part[f][lo:hi] = jnp.dot(
                cnt[ROWS * lo : ROWS * hi],
                rows[...].reshape(kt * 128, WIDTHS[f]),
                preferred_element_type=jnp.float32,
            ).reshape(hi - lo, ROWS, WIDTHS[f])
            return carry

        with scope(f"dot{f}{lo}"):
            lax.fori_loop(0, once, body, 0)

    def zcopy(way, f, m):
        return rc(
            send[f].at[way, m], got[f].at[way, m], z_s.at[0], z_r.at[f, m], (down, up)[way]
        )

    def zwait(f, m):
        ref = got[f].at[:, m]
        with scope(f"w{f}{m}"):
            rc(ref, ref, z_s.at[0], z_r.at[f, m], down).wait_recv()

    def reduce(f, r, some=(0, 1)):
        for m in (ROUNDS[r][i] for i in some):
            dist, half = MSG[m]
            if m >= 2:
                zwait(f, m - 2)
            for way in range(2):
                i = 2 * (4 - dist) - 1 + way
                value = part[f][i, HALF * half : HALF * (half + 1)]
                if m >= 2:
                    value = value + got[f][way, m - 2].astype(jnp.float32)
                send[f][way, m] = value.astype(jnp.bfloat16)
                zcopy(way, f, m).start()

    def finish(f):
        gather5(f + NC)
        dots(f, FAR)
        for half in range(2):
            zwait(f, 4 + half)
            rows = slice(HALF * half, HALF * (half + 1))
            total = (part[f][7, rows] + part[f][0, rows]) + (
                got[f][0, 4 + half].astype(jnp.float32) + got[f][1, 4 + half].astype(jnp.float32)
            )
            out_ref[rows, OFFS[f] : OFFS[f] + WIDTHS[f]] = total * (1.0 / LIST)

    start(ids_near[0])
    gather1(0)
    gather1(1)
    start(to_far)
    with scope("id1"):
        ids_near[3].wait_recv()
    join(0)
    start(ids_near[1])
    gather1(2)
    gather2(0)
    gather2(1)
    with scope("id2"):
        ids_near[4].wait_recv()
    start(ids_near[2])
    gather3(0)
    build(A, c)
    with scope("id3"):
        ids_near[5].wait_recv()
    build(A, 1 - c)
    gather3(1)
    gather2(2)
    gather1(3)
    gather1(4)
    to_far[0].wait_recv()
    ids_x[1, x] = ids_far[...]
    start(ids_away[0])
    build(B, c)
    gather4(0)
    build(B, 1 - c)
    gather5(0)
    dots(0, A)
    reduce(0, 0)
    to_far[1].wait_recv()
    for f in range(NC):
        xg[NC + f][c, y, x] = x_far[:, pl.ds(OFFS[f], WIDTHS[f])]
        gather1(NC + f)
    build(C, c)
    gather4(1)
    dots(0, B)
    gather5(1)
    dots(1, A)
    reduce(1, 0)
    gather3(2)
    gather2(3)
    reduce(0, 1)
    with scope("far"):
        ids_away[3].wait_recv()
    join(1)
    start(ids_away[1])
    build(C, 1 - c)
    dots(1, BC)
    reduce(1, 1)
    gather2(4)
    gather2(5)
    gather4(2)
    dots(0, C)
    reduce(0, 2)
    gather3(3)
    gather5(2)
    dots(2, A)
    reduce(2, 0)
    dots(2, BC)
    reduce(1, 2)
    gather2(6)
    gather3(4)
    reduce(2, 1, (0,))
    gather3(5)
    gather4(3)
    reduce(2, 1, (1,))
    gather2(7)
    with scope("id2far"):
        ids_away[4].wait_recv()
    start(ids_away[2])
    gather5(3)
    dots(3, ABC)
    reduce(3, 0)
    gather3(6)
    gather2(8)
    gather4(4)
    gather4(5)
    reduce(2, 2, (0,))
    gather5(4)
    dots(4, ABC)
    reduce(4, 0)
    reduce(2, 2, (1,))
    gather2(9)
    gather3(7)
    ids_away[5].wait_recv()
    build(FAR, c, 1)
    build(FAR, 1 - c, 1)
    reduce(3, 1)
    gather4(6)
    reduce(4, 1)
    finish(0)
    gather3(8)
    reduce(3, 2, (0,))
    gather3(9)
    reduce(3, 2, (1,))
    gather4(7)
    reduce(4, 2)
    gather4(8)
    finish(1)
    gather4(9)
    finish(2)
    finish(3)
    finish(4)

    with scope("drain"):
        for copies in (ids_near, ids_away):
            for step in (3, 4, 5):
                copies[step].wait_send()
        for cp in to_far:
            cp.wait_send()
        width = x_in.shape[1]
        depth = kt * 128
        for step, rows in enumerate(((ny - 1) * POS, 2 * ny * POS, ny * POS, nx * ny * POS)):
            ref = cnt.at[pl.ds(0, 2 * rows * width // depth)]
            rc(ref, ref, g_s.at[step], g_r.at[0, step], partner).wait_send()
        ref = cnt.at[pl.ds(0, 2 * len(MSG) * HALF * width // depth)]
        rc(ref, ref, z_s.at[0], z_r.at[0, 0], down).wait_send()


def local(nx, ny, pooled_grad, token_ids):
    width = pooled_grad.shape[1]
    dma = pltpu.SemaphoreType.DMA
    bf = jnp.bfloat16
    vmem = pltpu.VMEM
    return pl.pallas_call(
        functools.partial(kernel, nx, ny),
        out_shape=jax.ShapeDtypeStruct((ROWS, width), jnp.float32),
        in_specs=[pl.BlockSpec(memory_space=pl.ANY)] * 2,
        out_specs=pl.BlockSpec(memory_space=pltpu.VMEM),
        scratch_shapes=[
            vmem((POS, width), bf),
            vmem((POS, width), bf),
            vmem((LIST, POS), jnp.int32),
            vmem((LIST, 128), jnp.int32),
            vmem((2, nx, LIST, 128), jnp.int32),
            vmem((2, 2, ny, LIST, 128), jnp.int32),
            vmem((8 * ROWS, 2 * ny * 128), bf),
            *[vmem((8, ROWS, w), jnp.float32) for w in WIDTHS],
            *[vmem((2, len(MSG), HALF, w), bf) for w in WIDTHS],
            *[vmem((2, len(MSG), HALF, w), bf) for w in WIDTHS],
            *[vmem((2, ny, nx, POS, w), bf) for w in WIDTHS + WIDTHS],
            dma((2,)), dma((8,)), dma((8,)),
            dma((4,)), dma((2 * NC, 4)), dma((1,)), dma((NC, len(MSG))),
        ],
        compiler_params=pltpu.CompilerParams(
            collective_id=0, has_side_effects=True, vmem_limit_bytes=62 * 1024 * 1024
        ),
    )(pooled_grad, token_ids.T)


def solution(mesh, nx=4, ny=8):
    in_specs = (P(("dp", "vocab"), None), P(("dp", "vocab"), None))
    out_specs = P(("dp", "vocab"), None)
    return jax.shard_map(
        functools.partial(local, nx, ny), mesh=mesh, in_specs=in_specs, out_specs=out_specs, check_vma=False
    )
```

```python
import functools

import jax
import jax.numpy as jnp
from jax import lax
from jax.experimental import pallas as pl
from jax.experimental.pallas import tpu as pltpu
from jax.sharding import PartitionSpec as P

ROWS = 256
HALF = ROWS // 2
LIST = 16
POS = 32
WIDTHS = (128, 256, 256, 256, 128)
OFFS = tuple(sum(WIDTHS[:i]) for i in range(len(WIDTHS)))
NC = len(WIDTHS)
MESH = pl.DeviceIdType.MESH
MSG = ((3, 0), (3, 1), (2, 0), (2, 1), (1, 0), (1, 1))
ROUNDS = ((0, 1), (2, 3), (4, 5))
BLOCKS = (0, 5, 3, 6, 2, 7, 1, 0)
FAR, A, B, C, BC, ABC = (0, 1), (1, 3), (3, 5), (5, 8), (3, 8), (1, 8)


def kernel(nx, ny, x_hbm, ids_hbm, out_ref, x_in, x_far, ids_in, ids_far, ids_x, ids_g, cnt, *rest):
    part, send, got = (rest[NC * i : NC * (i + 1)] for i in range(3))
    xg = rest[3 * NC : 5 * NC]
    in_sem, id_s, id_r, g_s, g_r, z_s, z_r = rest[5 * NC :]
    scope = jax.named_scope
    d = lax.axis_index("dp")
    v = lax.axis_index("vocab")
    c = v % 2
    y = (v // 2) % ny
    x = v // (2 * ny)

    def at(xx, yy, cc):
        return (d, (xx * ny + yy) * 2 + cc)

    far_first = [sorted(range(1, n), key=lambda k, n=n: -min(k, n - k)) for n in (nx, ny)]
    xs = [lax.rem(x + k, nx) for k in range(nx)]
    ys = [lax.rem(y + k, ny) for k in range(ny)]
    partner = at(x, y, 1 - c)
    down = (lax.rem(d + 7, 8), v)
    up = (lax.rem(d + 1, 8), v)
    far = (lax.rem(d + 4, 8), v)

    cp_ids = pltpu.make_async_copy(ids_hbm, ids_in, in_sem.at[0])
    cp_x = pltpu.make_async_copy(x_hbm, x_in, in_sem.at[1])
    cp_ids.start()
    cp_x.start()

    peers = [at(x, ys[k], c) for k in range(1, ny)] + [at(xs[k], y, c) for k in range(1, nx)]
    peers += [partner, down, up, far]
    barrier = pltpu.get_barrier_semaphore()
    for peer in peers:
        pl.semaphore_signal(barrier, inc=1, device_id=peer, device_id_type=MESH)
    cp_ids.wait()
    ids_x[0, x] = jnp.concatenate([ids_in[...]] * nx, axis=1)
    cp_x.wait()
    for f in range(NC):
        xg[f][c, y, x] = x_in[:, pl.ds(OFFS[f], WIDTHS[f])]
    with scope("barrier"):
        pl.semaphore_wait(barrier, len(peers))

    def rc(src, dst, ss, rs, dev):
        return pltpu.make_async_remote_copy(
            src_ref=src, dst_ref=dst, send_sem=ss, recv_sem=rs, device_id=dev, device_id_type=MESH
        )

    def start(copies):
        for cp in copies:
            cp.start()

    def whole(ref, i):
        return rc(ref, ref, id_s.at[i], id_r.at[i], partner)

    def along_y(f):
        src = (x_in if f < NC else x_far).at[:, pl.ds(OFFS[f % NC], WIDTHS[f % NC])]
        return [
            rc(src, xg[f].at[c, y, x], g_s.at[0], g_r.at[f, 0], at(x, ys[k], c)) for k in far_first[1]
        ]

    def along_x(f):
        ref = xg[f].at[c, :, x]
        return [rc(ref, ref, g_s.at[1], g_r.at[f, 1], at(xs[k], y, c)) for k in (1, nx - 1)]

    def relay(f):
        lo = xg[f].at[c, pl.ds(0, ny // 2), xs[nx - 1]]
        hi = xg[f].at[c, pl.ds(ny // 2, ny // 2), xs[1]]
        return [
            rc(lo, lo, g_s.at[2], g_r.at[f, 2], at(xs[1], y, c)),
            rc(hi, hi, g_s.at[2], g_r.at[f, 2], at(xs[nx - 1], y, c)),
        ]

    def across(f, k):
        ref = xg[f].at[c, :, xs[k]]
        return rc(ref, ref, g_s.at[3], g_r.at[f, 3], partner)

    def all_of(f, step):
        ref = (
            xg[f].at[c, pl.ds(0, ny - 1), 0],
            xg[f].at[c, :, pl.ds(0, 2)],
            xg[f].at[c, :, 0],
            xg[f].at[c],
        )[step]
        return rc(ref, ref, g_s.at[step], g_r.at[f, step], partner)

    def gather1(f):
        start(along_y(f))

    def gather2(f):
        with scope(f"g2_{f}"):
            all_of(f, 0).wait_recv()
        start(along_x(f))
        across(f, 0).start()

    def gather3(f):
        with scope(f"g3_{f}"):
            all_of(f, 1).wait_recv()
        start(relay(f))
        across(f, 1).start()
        across(f, nx - 1).start()

    def gather4(f):
        with scope(f"g4_{f}"):
            all_of(f, 2).wait_recv()
        across(f, 2).start()

    def gather5(f):
        with scope(f"g5_{f}"):
            all_of(f, 3).wait_recv()

    def ids_copies(e):
        near = ids_x.at[e, x]
        line = ids_g.at[e, c, y]
        plane = ids_g.at[e, c]
        k = 3 * e
        return (
            [rc(near, near, id_s.at[k], id_r.at[k], at(xs[i], y, c)) for i in far_first[0]],
            [rc(line, line, id_s.at[k + 1], id_r.at[k + 1], at(x, ys[i], c)) for i in far_first[1]],
            [rc(plane, plane, id_s.at[k + 2], id_r.at[k + 2], partner)],
            whole(ids_x.at[e, pl.ds(0, nx - 1)], k),
            whole(ids_g.at[e, c, pl.ds(0, ny - 1)], k + 1),
            whole(plane, k + 2),
        )

    ids_near, ids_away = ids_copies(0), ids_copies(1)

    def join(e):
        lane = lax.broadcasted_iota(jnp.int32, (LIST, 128), 1) // POS
        both = ids_x[e, 0]
        for k in range(1, nx):
            both = jnp.where(lane == k, ids_x[e, k], both)
        ids_g[e, c, y] = both

    to_far = (
        rc(ids_x.at[0, x], ids_far, id_s.at[6], id_r.at[6], far),
        rc(x_in, x_far, id_s.at[7], id_r.at[7], far),
    )

    blocks = [lax.rem(d + k, 8) for k in BLOCKS]
    kt = 2 * ny

    def build(g, core, e=0):
        lo, hi = g

        def tile(k, _):
            ids = ids_g[e, core, k]
            t = core * ny + k
            low = ids & (ROWS - 1)
            block = ids >> 8
            word = low & 31
            bit = jnp.left_shift(1, (low >> 5) * 4)
            wide = lax.broadcasted_iota(jnp.int32, (32, 128), 0)
            vals = [jnp.where(block == blocks[i] * (2 * nx * ny) + v, bit, 0) for i in range(lo, hi)]
            acc = [[jnp.zeros((32, 128), jnp.int32) for _ in range(2)] for _ in vals]
            for j in range(LIST):
                eq = jnp.broadcast_to(word[j : j + 1], (32, 128)) == wide
                for n, val in enumerate(vals):
                    acc[n][j // 8] += jnp.where(eq, jnp.broadcast_to(val[j : j + 1], (32, 128)), 0)
            nib = 0x0F0F0F0F
            for n in range(len(vals)):
                a, b = acc[n]
                both = ((a & nib) + (b & nib), ((a >> 4) & nib) + ((b >> 4) & nib))
                for s in range(8):
                    count = (both[s % 2] >> (8 * (s // 2))) & 255
                    cnt[pl.ds(ROWS * (lo + n) + 32 * s, 32), pl.ds(pl.multiple_of(t * 128, 128), 128)] = count.astype(
                        jnp.float32
                    ).astype(jnp.bfloat16)
            return 0

        with scope(f"build{lo}"):
            lax.fori_loop(0, ny, tile, 0)

    once = jnp.minimum(d + 1, 1)

    def dots(f, g):
        lo, hi = g
        rows = xg[f + NC] if g is FAR else xg[f]

        def body(_, carry):
            part[f][lo:hi] = jnp.dot(
                cnt[ROWS * lo : ROWS * hi],
                rows[...].reshape(kt * 128, WIDTHS[f]),
                preferred_element_type=jnp.float32,
            ).reshape(hi - lo, ROWS, WIDTHS[f])
            return carry

        with scope(f"dot{f}{lo}"):
            lax.fori_loop(0, once, body, 0)

    def zcopy(way, f, m):
        return rc(
            send[f].at[way, m], got[f].at[way, m], z_s.at[0], z_r.at[f, m], (down, up)[way]
        )

    def zwait(f, m):
        ref = got[f].at[:, m]
        with scope(f"w{f}{m}"):
            rc(ref, ref, z_s.at[0], z_r.at[f, m], down).wait_recv()

    def reduce(f, r, some=(0, 1)):
        for m in (ROUNDS[r][i] for i in some):
            dist, half = MSG[m]
            if m >= 2:
                zwait(f, m - 2)
            for way in range(2):
                i = 2 * (4 - dist) - 1 + way
                value = part[f][i, HALF * half : HALF * (half + 1)]
                if m >= 2:
                    value = value + got[f][way, m - 2].astype(jnp.float32)
                send[f][way, m] = value.astype(jnp.bfloat16)
                zcopy(way, f, m).start()

    def finish(f):
        gather5(f + NC)
        dots(f, FAR)
        for half in range(2):
            zwait(f, 4 + half)
            rows = slice(HALF * half, HALF * (half + 1))
            total = (part[f][7, rows] + part[f][0, rows]) + (
                got[f][0, 4 + half].astype(jnp.float32) + got[f][1, 4 + half].astype(jnp.float32)
            )
            out_ref[rows, OFFS[f] : OFFS[f] + WIDTHS[f]] = total * (1.0 / LIST)

    start(ids_near[0])
    gather1(0)
    gather1(1)
    start(to_far)
    with scope("id1"):
        ids_near[3].wait_recv()
    join(0)
    start(ids_near[1])
    gather1(2)
    gather2(0)
    gather2(1)
    with scope("id2"):
        ids_near[4].wait_recv()
    start(ids_near[2])
    gather3(0)
    build(A, c)
    with scope("id3"):
        ids_near[5].wait_recv()
    build(A, 1 - c)
    gather3(1)
    gather2(2)
    gather1(3)
    gather1(4)
    to_far[0].wait_recv()
    ids_x[1, x] = ids_far[...]
    start(ids_away[0])
    build(B, c)
    gather4(0)
    build(B, 1 - c)
    gather5(0)
    dots(0, A)
    reduce(0, 0)
    to_far[1].wait_recv()
    for f in range(NC):
        xg[NC + f][c, y, x] = x_far[:, pl.ds(OFFS[f], WIDTHS[f])]
        gather1(NC + f)
    dots(0, B)
    gather4(1)
    gather5(1)
    dots(1, A)
    reduce(1, 0)
    gather3(2)
    gather2(3)
    reduce(0, 1)
    with scope("far"):
        ids_away[3].wait_recv()
    join(1)
    start(ids_away[1])
    build(C, c)
    dots(1, B)
    reduce(1, 1, (0,))
    gather4(2)
    reduce(1, 1, (1,))
    gather5(2)
    dots(2, A)
    reduce(2, 0)
    gather2(4)
    gather2(5)
    build(C, 1 - c)
    dots(0, C)
    reduce(0, 2)
    gather3(3)
    dots(1, C)
    reduce(1, 2)
    dots(2, BC)
    gather2(6)
    gather3(4)
    reduce(2, 1, (0,))
    gather3(5)
    gather4(3)
    reduce(2, 1, (1,))
    gather2(7)
    with scope("id2far"):
        ids_away[4].wait_recv()
    start(ids_away[2])
    gather5(3)
    dots(3, ABC)
    reduce(3, 0)
    gather3(6)
    gather2(8)
    gather4(4)
    gather4(5)
    reduce(2, 2, (0,))
    gather5(4)
    dots(4, ABC)
    reduce(4, 0)
    reduce(2, 2, (1,))
    gather2(9)
    gather3(7)
    ids_away[5].wait_recv()
    build(FAR, c, 1)
    build(FAR, 1 - c, 1)
    reduce(3, 1)
    gather4(6)
    reduce(4, 1)
    finish(0)
    gather3(8)
    reduce(3, 2, (0,))
    gather3(9)
    reduce(3, 2, (1,))
    gather4(7)
    reduce(4, 2)
    gather4(8)
    finish(1)
    gather4(9)
    finish(2)
    finish(3)
    finish(4)

    with scope("drain"):
        for copies in (ids_near, ids_away):
            for step in (3, 4, 5):
                copies[step].wait_send()
        for cp in to_far:
            cp.wait_send()
        width = x_in.shape[1]
        depth = kt * 128
        for step, rows in enumerate(((ny - 1) * POS, 2 * ny * POS, ny * POS, nx * ny * POS)):
            ref = cnt.at[pl.ds(0, 2 * rows * width // depth)]
            rc(ref, ref, g_s.at[step], g_r.at[0, step], partner).wait_send()
        ref = cnt.at[pl.ds(0, 2 * len(MSG) * HALF * width // depth)]
        rc(ref, ref, z_s.at[0], z_r.at[0, 0], down).wait_send()


def local(nx, ny, pooled_grad, token_ids):
    width = pooled_grad.shape[1]
    dma = pltpu.SemaphoreType.DMA
    bf = jnp.bfloat16
    vmem = pltpu.VMEM
    return pl.pallas_call(
        functools.partial(kernel, nx, ny),
        out_shape=jax.ShapeDtypeStruct((ROWS, width), jnp.float32),
        in_specs=[pl.BlockSpec(memory_space=pl.ANY)] * 2,
        out_specs=pl.BlockSpec(memory_space=pltpu.VMEM),
        scratch_shapes=[
            vmem((POS, width), bf),
            vmem((POS, width), bf),
            vmem((LIST, POS), jnp.int32),
            vmem((LIST, 128), jnp.int32),
            vmem((2, nx, LIST, 128), jnp.int32),
            vmem((2, 2, ny, LIST, 128), jnp.int32),
            vmem((8 * ROWS, 2 * ny * 128), bf),
            *[vmem((8, ROWS, w), jnp.float32) for w in WIDTHS],
            *[vmem((2, len(MSG), HALF, w), bf) for w in WIDTHS],
            *[vmem((2, len(MSG), HALF, w), bf) for w in WIDTHS],
            *[vmem((2, ny, nx, POS, w), bf) for w in WIDTHS + WIDTHS],
            dma((2,)), dma((8,)), dma((8,)),
            dma((4,)), dma((2 * NC, 4)), dma((1,)), dma((NC, len(MSG))),
        ],
        compiler_params=pltpu.CompilerParams(
            collective_id=0, has_side_effects=True, vmem_limit_bytes=62 * 1024 * 1024
        ),
    )(pooled_grad, token_ids.T)


def solution(mesh, nx=4, ny=8):
    in_specs = (P(("dp", "vocab"), None), P(("dp", "vocab"), None))
    out_specs = P(("dp", "vocab"), None)
    return jax.shard_map(
        functools.partial(local, nx, ny), mesh=mesh, in_specs=in_specs, out_specs=out_specs, check_vma=False
    )
```
